256 devices in a mesh: gx: 8 (over z), gy: 8 (over x, y_lo), gz: 4 (over y_hi, core).
Axes of the slice: x: 4, y: 4 (y_hi: 2, y_lo: 2; y = y_hi * 2 + y_lo), z: 8, core: 2. Of those that a mesh axis runs over, the one named last changes fastest.
Arguments:
- fields_now: float32 [24, 64, 64, 512], P(None, 'gx', 'gy', 'gz'), may hold values from -6 to 6
- parent: float32 [24, 64, 64, 512], P(None, 'gx', 'gy', 'gz'), may hold values from -6 to 6
- advect: float32 [3, 24, 24], replicated, may hold values from -0.75 to 0.75
- diffuse: float32 [3, 24, 24], replicated, may hold values from -0.25 to 0.25
- box_shift: int32 [3], replicated, may hold values from 1 to 4
Outputs:
- section_slope: float32 [24, 64, 64, 512], P(None, 'gx', 'gy', 'gz')
- section_value: float32 [24, 64, 64, 512], P(None, 'gx', 'gy', 'gz')
The draws below stay inside these ranges and needn't reach their ends.
All inputs are finite; a program needn't handle non-finite values.
Results may differ from the reference program's by a relative error of at most 0.0001.
Values sent between devices are 32-bit elements; how exact they have to be, the bound alone decides.
A program may use at most 64 MiB of HBM per device.

```python
import jax
import jax.numpy as jnp
from jax import lax

F = 24
NX = 64
NY = 64
NZ = 512


def level_of(rng, shape, shards, low, top_value):
    gain, own = 1.0, jax.random.fold_in(rng, 6)
    for dim, parts in shards:
        heights = jnp.exp(jax.random.uniform(jax.random.fold_in(own, dim), (parts,), jnp.float32, low / len(shards), top_value / len(shards)))
        gain = gain * jnp.repeat(heights, shape[dim] // parts).reshape([-1 if axis == dim else 1 for axis in range(len(shape))])
    return gain


def scatter_about(own_key, shape, width, most, pieces=(), held_as=jnp.bfloat16):
    values = width * jax.random.normal(own_key, shape, jnp.float32)
    if pieces:
        values = values * level_of(own_key, shape, pieces, -0.22, 0.18)
    return jnp.clip(values, -most, most).astype(held_as)


def setup_inputs(seed: int = 0) -> dict:
    keys = jax.random.split(jax.random.key(seed), 6)
    fields_now = scatter_about(keys[0], (F, NX, NY, NZ), 1.0, 6.0, ((1, 8), (2, 8), (3, 4)), jnp.float32)
    parent = scatter_about(keys[1], (F, NX, NY, NZ), 1.0, 6.0, ((1, 8), (2, 8), (3, 4)), jnp.float32)
    advect = scatter_about(keys[2], (3, F, F), (3 * F) ** -0.5, 0.75, (), jnp.float32)
    diffuse = scatter_about(keys[3], (3, F, F), (27 * F) ** -0.5, 0.25, (), jnp.float32)
    box_shift = jax.random.randint(keys[4], (3,), 1, 5).astype(jnp.int32)
    return {"fields_now": fields_now, "parent": parent, "advect": advect, "diffuse": diffuse, "box_shift": box_shift}


dissipation = 1.0
half_step = 0.125


def line_terms(padded_line, axis):
    length = padded_line.shape[axis] - 6

    def take_at(offset):
        return lax.slice_in_dim(padded_line, 3 + offset, 3 + offset + length, axis=axis)

    first_diff = (take_at(-2) - 8.0 * take_at(-1) + 8.0 * take_at(1) - take_at(2)) / 12.0
    second_diff = (-take_at(-2) + 16.0 * take_at(-1) - 30.0 * take_at(0) + 16.0 * take_at(1) - take_at(2)) / 12.0
    sixth_diff = (take_at(-3) - 6.0 * take_at(-2) + 15.0 * take_at(-1) - 20.0 * take_at(0)
                  + 15.0 * take_at(1) - 6.0 * take_at(2) + take_at(3))
    return first_diff, second_diff, sixth_diff


def mix_fields(matrix, field):
    flat = field.reshape(field.shape[0], -1)
    return jnp.dot(matrix, flat, precision=lax.Precision.HIGHEST,
                   preferred_element_type=jnp.float32).reshape(field.shape)


def center_crop(padded, axis):
    window = [slice(None)] * 4
    for other in (1, 2, 3):
        if other != axis:
            window[other] = slice(3, padded.shape[other] - 3)
    return padded[tuple(window)]


def axis_terms(line, axis, advect, diffuse):
    first_diff, second_diff, sixth_diff = line_terms(line, axis)
    coupled = mix_fields(advect[axis - 1], first_diff) + mix_fields(diffuse[axis - 1], second_diff)
    return coupled, sixth_diff


def whole_terms(padded, advect, diffuse):
    linear, smooth = axis_terms(center_crop(padded, 1), 1, advect, diffuse)
    for axis in (2, 3):
        coupled, sixth_diff = axis_terms(center_crop(padded, axis), axis, advect, diffuse)
        linear = linear + coupled
        smooth = smooth + sixth_diff
    return linear, smooth


def finish(new_box, linear, smooth):
    lapse_factor = 1.0 + 0.25 * jnp.tanh(new_box[0])
    section_slope = lapse_factor * linear + (dissipation / 64.0) * smooth
    section_value = new_box + half_step * section_slope
    return section_slope, section_value


def reference(fields_now, parent, advect, diffuse, box_shift):
    room = jnp.pad(fields_now, ((0, 0), (0, 4), (0, 4), (0, 4)))
    anchor = jnp.zeros((), jnp.int32)
    moved_cells = lax.dynamic_slice(room, (anchor, box_shift[0], box_shift[1], box_shift[2]), fields_now.shape)
    keep_mask = None
    for axis in (1, 2, 3):
        shape_one = [1, 1, 1, 1]
        shape_one[axis] = fields_now.shape[axis]
        position = lax.broadcasted_iota(jnp.int32, tuple(shape_one), axis)
        inside = position + box_shift[axis - 1] < fields_now.shape[axis]
        keep_mask = inside if keep_mask is None else keep_mask & inside
    new_box = jnp.where(keep_mask, moved_cells, parent)
    padded = jnp.pad(new_box, ((0, 0), (3, 3), (3, 3), (3, 3)))
    linear, smooth = whole_terms(padded, advect, diffuse)
    return finish(new_box, linear, smooth)
```

```python
import jax
import jax.numpy as jnp
from jax import lax
from jax.experimental import pallas as pl
from jax.experimental.pallas import tpu as pltpu
from jax.sharding import PartitionSpec as P

MESH = pl.DeviceIdType.MESH
F32, BF16 = jnp.float32, jnp.bfloat16
GROUPS = 3
NX, NY, NZ = 8, 8, 128


def lane_iota():
    return lax.broadcasted_iota(jnp.int32, (8, NZ), 1)


def kernel(shift, now_hbm, parent_hbm, advect, diffuse, slope_hbm, value_hbm, *scratch):
    scratch = list(scratch)

    def take(count):
        got = scratch[:count]
        del scratch[:count]
        return got

    now_v, parent_v, slope_v, value_v, acc, mixed, weights, weight_f32 = take(8)
    raw = [take(2) for _ in range(GROUPS)]
    moved = take(GROUPS)
    zs, zr = take(GROUPS), take(GROUPS)
    box = take(GROUPS)
    arm_sd, arm_su, arm_rd, arm_ru = take(GROUPS), take(GROUPS), take(GROUPS), take(GROUPS)
    load_sem, store_sem, a_send, a_recv, b_send, b_recv, z_send, z_recv, arm_send, arm_recv = take(10)

    gx, gy, gz = lax.axis_index("gx"), lax.axis_index("gy"), lax.axis_index("gz")
    ex, ey, ez = lax.axis_size("gx"), lax.axis_size("gy"), lax.axis_size("gz")
    place = {"gx": gx, "gy": gy, "gz": gz}
    has_low = {"gx": gx > 0, "gy": gy > 0, "gz": gz > 0}
    has_high = {"gx": gx < ex - 1, "gy": gy < ey - 1, "gz": gz < ez - 1}
    s0, s1, s2 = shift[0], shift[1], shift[2]

    def remote(src, dst, send, recv, axis, step):
        return pltpu.make_async_remote_copy(
            src_ref=src, dst_ref=dst, send_sem=send, recv_sem=recv,
            device_id={axis: place[axis] + step}, device_id_type=MESH)

    loads = [pltpu.make_async_copy(now_hbm.at[pl.ds(8 * c, 8)], now_v.at[pl.ds(8 * c, 8)], load_sem.at[c])
             for c in range(GROUPS)]
    loads.append(pltpu.make_async_copy(parent_hbm, parent_v, load_sem.at[GROUPS]))
    for load in loads:
        load.start()

    barrier = pltpu.get_barrier_semaphore()
    for axis in ("gx", "gy", "gz"):
        for present, step in ((has_low[axis], -1), (has_high[axis], 1)):
            @pl.when(present)
            def _():
                pl.semaphore_signal(barrier, inc=1, device_id={axis: place[axis] + step}, device_id_type=MESH)

    for c in range(GROUPS):
        loads[c].wait()
        for h in range(2):
            def turn(x, carry, c=c, h=h):
                raw[c][h][x, 0:8] = jnp.swapaxes(now_v[8 * c:8 * c + 8, 4 * h + x], 0, 1)
                return carry
            lax.fori_loop(0, 4, turn, 0)

    peers = [has[axis].astype(jnp.int32) for axis in ("gx", "gy", "gz") for has in (has_low, has_high)]
    pl.semaphore_wait(barrier, sum(peers))

    a_copies = [[remote(raw[c][h].at[:, 0:4], raw[c][h].at[:, 8:12], a_send.at[c, h], a_recv.at[c, h], "gy", -1)
                 for h in range(2)] for c in range(GROUPS)]
    b_copies = [remote(moved[c].at[0:4], moved[c].at[8:12], b_send.at[c], b_recv.at[c], "gx", -1) for c in range(GROUPS)]
    z_copies = [remote(zs[c], zr[c], z_send.at[c], z_recv.at[c], "gz", -1) for c in range(GROUPS)]

    @pl.when(has_low["gy"])
    def _():
        for h in range(2):
            for c in range(GROUPS):
                a_copies[c][h].start()

    edges = (
        ("gx", has_low, lambda r: r.at[0:3, 3:11]), ("gx", has_high, lambda r: r.at[11:14, 3:11]),
        ("gy", has_low, lambda r: r.at[3:11, 0:3]), ("gy", has_high, lambda r: r.at[3:11, 11:14]))
    for axis, has, view in edges:
        @pl.when(jnp.logical_not(has[axis]))
        def _():
            for c in range(GROUPS):
                ref = view(box[c])
                ref[...] = jnp.zeros(ref.shape, F32)

    @pl.when(jnp.logical_not(has_low["gz"]))
    def _():
        for c in range(GROUPS):
            arm_rd[c][...] = jnp.zeros(arm_rd[c].shape, F32)

    @pl.when(jnp.logical_not(has_high["gz"]))
    def _():
        for c in range(GROUPS):
            arm_ru[c][...] = jnp.zeros(arm_ru[c].shape, F32)

    for c in range(GROUPS):
        for k in range(12):
            q = k % 6
            source = advect if q < 3 else diffuse
            weight_f32[:, 8 * k:8 * k + 8] = source[q % 3, :, 8 * c:8 * c + 8] * (1.0 / 12.0)
        full = weight_f32[...]
        high = full.astype(BF16).astype(F32)
        weights[c] = jnp.concatenate([high, full - high], axis=0).astype(BF16)

    def shift_y(c, h):
        def body(x, carry):
            moved[c][4 * h + x] = raw[c][h][x, pl.ds(s1, 8)]
            return carry
        lax.fori_loop(0, 4, body, 0)

    for c in range(GROUPS):
        @pl.when(has_high["gy"])
        def _():
            a_copies[c][0].wait_recv()
        shift_y(c, 0)

        @pl.when(has_low["gx"])
        def _():
            b_copies[c].start()

    loads[GROUPS].wait()

    lane = lane_iota()
    group = lane // 4

    for c in range(GROUPS):
        @pl.when(has_high["gy"])
        def _():
            a_copies[c][1].wait_recv()
        shift_y(c, 1)

        @pl.when(has_high["gx"])
        def _():
            b_copies[c].wait_recv()

        for half in range(2):
            def pack(x, packed, c=c, half=half):
                for y in range(8):
                    tile = moved[c][4 * half + x + s0, y]
                    at = 8 * x + y
                    packed = jnp.where(group == at, pltpu.roll(tile, 4 * at, 1), packed)
                return packed
            zs[c][half] = lax.fori_loop(0, 4, pack, jnp.zeros((8, NZ), F32))

        @pl.when(has_low["gz"])
        def _():
            z_copies[c].start()

    def arm(c, k, src, dst, axis, step):
        return remote(src, dst, arm_send.at[c, k], arm_recv.at[c, k], axis, step)

    arms = [[
        arm(c, 0, box[c].at[3:11, 3:6], box[c].at[3:11, 11:14], "gy", -1),
        arm(c, 1, box[c].at[3:11, 8:11], box[c].at[3:11, 0:3], "gy", 1),
        arm(c, 2, box[c].at[3:6, 3:11], box[c].at[11:14, 3:11], "gx", -1),
        arm(c, 3, box[c].at[8:11, 3:11], box[c].at[0:3, 3:11], "gx", 1),
        arm(c, 4, arm_sd[c], arm_ru[c], "gz", -1),
        arm(c, 5, arm_su[c], arm_rd[c], "gz", 1)] for c in range(GROUPS)]
    arm_axes = ("gy", "gy", "gx", "gx", "gz", "gz")

    for c in range(GROUPS):
        @pl.when(has_high["gz"])
        def _():
            z_copies[c].wait_recv()

        for half in range(2):
            def build(x, packed, c=c, half=half):
                low, high = packed
                parent_tiles = jnp.swapaxes(parent_v[8 * c:8 * c + 8, 4 * half + x], 0, 1)
                lanes_moved = zr[c][half]
                for y in range(8):
                    at = 8 * x + y
                    own = pltpu.roll(moved[c][4 * half + x + s0, y], NZ - s2, 1)
                    beyond = pltpu.roll(lanes_moved, lax.rem(2 * NZ - s2 - 4 * at, NZ), 1)
                    inside = (gx * NX + 4 * half + x + s0 < ex * NX) & (gy * NY + y + s1 < ey * NY)
                    limit = jnp.where(inside, ez * NZ - gz * NZ - s2, 0)
                    tile = jnp.where(lane < NZ - s2, own, beyond)
                    tile = jnp.where(lane < limit, tile, parent_tiles[y])
                    box[c][3 + 4 * half + x, 3 + y] = tile
                    low = jnp.where(group == at, pltpu.roll(tile, 4 * at, 1), low)
                    high = jnp.where(group == at, pltpu.roll(tile, lax.rem(4 * at + 4, NZ), 1), high)
                return low, high
            zero = jnp.zeros((8, NZ), F32)
            low, high = lax.fori_loop(0, 4, build, (zero, zero))
            arm_sd[c][half] = low
            arm_su[c][half] = high

        for k in range(6):
            @pl.when((has_low if k % 2 == 0 else has_high)[arm_axes[k]])
            def _():
                arms[c][k].start()

    for c in range(GROUPS):
        for k in range(6):
            @pl.when((has_high if k % 2 == 0 else has_low)[arm_axes[k]])
            def _():
                arms[c][k].wait_recv()

        def line(m3, m2, m1, u0, p1, p2, p3):
            d1, d2 = p1 - m1, p2 - m2
            t1, t2, t3 = p1 + m1, p2 + m2, p3 + m3
            first = 8.0 * d1 - d2
            second = 16.0 * t1 - t2 - 30.0 * u0
            sixth = t3 - 6.0 * t2 + 15.0 * t1
            return first, second, sixth

        for half in range(2):
            def work(x4, carry, c=c, half=half):
                x = 4 * half + x4
                column = [box[c][3 + x, y] for y in range(14)]
                low_pack, high_pack = arm_rd[c][half], arm_ru[c][half]
                for y in range(8):
                    at = 8 * x4 + y
                    u0 = column[3 + y]
                    ends = jnp.where(lane < 64, pltpu.roll(high_pack, lax.rem(NZ - 4 * at, NZ), 1),
                                     pltpu.roll(low_pack, lax.rem(2 * NZ - 4 - 4 * at, NZ), 1))
                    taps = []
                    for o in (3, 2, 1):
                        taps.append(pltpu.roll(jnp.where(lane >= NZ - o, ends, u0), o, 1))
                    taps.append(u0)
                    for o in (1, 2, 3):
                        taps.append(pltpu.roll(jnp.where(lane < o, ends, u0), NZ - o, 1))
                    fz, sz, qz = line(*taps)
                    fy, sy, qy = line(*column[y:y + 7])
                    fx, sx, qx = line(*[box[c][x + o, 3 + y] for o in range(3)], u0,
                                      *[box[c][x + o, 3 + y] for o in range(4, 7)])
                    slope_v[8 * c + y, x] = qx + qy + qz - 60.0 * u0
                    full = jnp.concatenate([fx, fy, fz, sx, sy, sz], axis=0)
                    top = full.astype(BF16)
                    mixed[0:48, 128 * y:128 * y + 128] = top
                    mixed[48:96, 128 * y:128 * y + 128] = (full - top.astype(F32)).astype(BF16)
                product = jnp.dot(weights[c], mixed[...], preferred_element_type=F32)
                product = product[0:24] + product[24:48]
                if c == 0:
                    acc[x] = product
                else:
                    acc[x] = acc[x] + product
                return carry
            lax.fori_loop(0, 4, work, 0)

    stores = []
    for ref, hbm, k in ((slope_v, slope_hbm, 0), (value_v, value_hbm, 1)):
        stores.append(pltpu.make_async_copy(ref, hbm, store_sem.at[k]))

    def close(x, carry):
        factors = [1.0 + 0.25 * jnp.tanh(box[0][3 + x, 3 + y][0:1]) for y in range(8)]
        for c in range(GROUPS):
            slopes, values = [], []
            for y in range(8):
                slope = factors[y] * acc[x, 8 * c:8 * c + 8, 128 * y:128 * y + 128] + slope_v[8 * c + y, x] * (1.0 / 64.0)
                slopes.append(slope)
                values.append(box[c][3 + x, 3 + y] + 0.125 * slope)
            slope_v[8 * c:8 * c + 8, x] = jnp.swapaxes(jnp.stack(slopes), 0, 1)
            value_v[8 * c:8 * c + 8, x] = jnp.swapaxes(jnp.stack(values), 0, 1)
        return carry
    lax.fori_loop(0, NX, close, 0)
    for store in stores:
        store.start()

    @pl.when(has_low["gy"])
    def _():
        for c in range(GROUPS):
            for h in range(2):
                a_copies[c][h].wait_send()

    @pl.when(has_low["gx"])
    def _():
        for c in range(GROUPS):
            b_copies[c].wait_send()

    @pl.when(has_low["gz"])
    def _():
        for c in range(GROUPS):
            z_copies[c].wait_send()
    for k in range(6):
        @pl.when((has_low if k % 2 == 0 else has_high)[arm_axes[k]])
        def _():
            for c in range(GROUPS):
                arms[c][k].wait_send()
    for store in stores:
        store.wait()


def local(fields_now, parent, advect, diffuse, box_shift):
    shape = jax.ShapeDtypeStruct(fields_now.shape, F32)
    whole = pltpu.VMEM(fields_now.shape, F32)
    packed = [pltpu.VMEM((2, 8, NZ), F32)] * GROUPS
    dma = pltpu.SemaphoreType.DMA
    scratch = [
        whole, whole, whole, whole,
        pltpu.VMEM((NX, 24, NY * NZ), F32), pltpu.VMEM((96, NY * NZ), BF16),
        pltpu.VMEM((GROUPS, 48, 96), BF16), pltpu.VMEM((24, 96), F32),
        *[pltpu.VMEM((4, 12, 8, NZ), F32)] * (2 * GROUPS),
        *[pltpu.VMEM((12, 8, 8, NZ), F32)] * GROUPS,
        *packed, *packed,
        *[pltpu.VMEM((14, 14, 8, NZ), F32)] * GROUPS,
        *packed, *packed, *packed, *packed,
        dma((GROUPS + 1,)), dma((2,)), dma((GROUPS, 2)), dma((GROUPS, 2)), dma((GROUPS,)), dma((GROUPS,)),
        dma((GROUPS,)), dma((GROUPS,)), dma((GROUPS, 6)), dma((GROUPS, 6)),
    ]
    hbm, vmem = pl.BlockSpec(memory_space=pl.ANY), pl.BlockSpec(memory_space=pltpu.VMEM)
    return pl.pallas_call(
        kernel,
        out_shape=(shape, shape),
        in_specs=[pl.BlockSpec(memory_space=pltpu.SMEM), hbm, hbm, vmem, vmem],
        out_specs=(hbm, hbm),
        scratch_shapes=scratch,
        compiler_params=pltpu.CompilerParams(collective_id=0, has_side_effects=True),
        name="section",
    )(box_shift, fields_now, parent, advect, diffuse)


def solution(mesh):
    return jax.shard_map(
        local,
        mesh=mesh,
        in_specs=(P(None, "gx", "gy", "gz"), P(None, "gx", "gy", "gz"), P(), P(), P()),
        out_specs=(P(None, "gx", "gy", "gz"), P(None, "gx", "gy", "gz")),
        check_vma=False,
    )
```

```python
import functools

import jax
import jax.numpy as jnp
from jax import lax
from jax.experimental import pallas as pl
from jax.experimental.pallas import tpu as pltpu
from jax.sharding import PartitionSpec as P

MESH = pl.DeviceIdType.MESH
F32, BF16 = jnp.float32, jnp.bfloat16
GROUPS = 3
NX, NY, NZ = 8, 8, 128
AXES = ("gx", "gy", "gz")
LANE_PEERS = ((0, 0, 1), (0, 1, 1), (1, 0, 1), (1, 1, 1))


def kernel(s1, shift_hbm, now_hbm, parent_hbm, advect_hbm, diffuse_hbm, slope_hbm, value_hbm, *scratch):
    scratch = list(scratch)

    def take(count):
        got = scratch[:count]
        del scratch[:count]
        return got

    shift, advect, diffuse, now_v, parent_v, slope_v, value_v, acc = take(8)
    mixed, weights, weight_f32, lanes_out, lanes_in = take(5)
    raw, above, box = take(GROUPS), take(GROUPS), take(GROUPS)
    arm_out, arm_low, arm_high = take(GROUPS), take(GROUPS), take(GROUPS)
    load_sem, store_sem, a_send, a_recv, b_send, b_recv, z_send, z_recv, arm_send, arm_recv = take(10)

    place = [lax.axis_index(axis) for axis in AXES]
    sizes = [lax.axis_size(axis) for axis in AXES]
    gx, gy, gz = place

    def exists(step):
        found = None
        for at, size, by in zip(place, sizes, step):
            if by:
                inside = (at < size - 1) if by > 0 else (at > 0)
                found = inside if found is None else found & inside
        return found

    def peer(step):
        return {axis: at + by for axis, at, by in zip(AXES, place, step) if by}

    def remote(src, dst, send, recv, step):
        return pltpu.make_async_remote_copy(
            src_ref=src, dst_ref=dst, send_sem=send, recv_sem=recv, device_id=peer(step), device_id_type=MESH)

    def opposite(step):
        return tuple(-by for by in step)

    barrier = pltpu.get_barrier_semaphore()
    steps = []
    for step in LANE_PEERS + ((0, 1, 0), (1, 0, 0)):
        steps += [step, opposite(step)]
    for step in steps:
        @pl.when(exists(step))
        def _():
            pl.semaphore_signal(barrier, inc=1, device_id=peer(step), device_id_type=MESH)

    loads = [pltpu.make_async_copy(now_hbm.at[pl.ds(8 * c, 8)], now_v.at[pl.ds(8 * c, 8)], load_sem.at[c])
             for c in range(GROUPS)]
    loads.append(pltpu.make_async_copy(shift_hbm, shift, load_sem.at[3]))
    loads.append(pltpu.make_async_copy(parent_hbm, parent_v, load_sem.at[4]))
    loads.append(pltpu.make_async_copy(advect_hbm, advect, load_sem.at[5]))
    loads.append(pltpu.make_async_copy(diffuse_hbm, diffuse, load_sem.at[6]))
    for load in loads:
        load.start()

    lane = lax.broadcasted_iota(jnp.int32, (8, NZ), 1)
    four, eight = lane // 4, lane // 8
    zero = jnp.zeros((8, NZ), F32)
    packed = (zero,) * NY
    for c in range(GROUPS):
        loads[c].wait()

        def turn(x, packed, c=c):
            tiles = jnp.swapaxes(now_v[8 * c:8 * c + 8, x], 0, 1)
            raw[c][x, 0:8] = tiles
            at = 3 * x + c
            return tuple(jnp.where(four == at, pltpu.roll(tiles[y], 4 * at, 1), packed[y]) for y in range(NY))
        packed = lax.fori_loop(0, NX, turn, packed, unroll=2)
    for y in range(NY):
        lanes_out[y] = packed[y]

    pl.semaphore_wait(barrier, sum(exists(step).astype(jnp.int32) for step in steps))

    lane_copies = []
    for k, (dx, dy, dz) in enumerate(LANE_PEERS):
        rows, start = (s1, 8) if dy else (8, 0)
        lane_copies.append(remote(lanes_out.at[0:rows], lanes_in.at[dx, start:start + rows],
                                  z_send.at[k], z_recv.at[k], (-dx, -dy, -dz)))
    a_copies = [[remote(raw[c].at[4 * h:4 * h + 4, 0:s1], raw[c].at[4 * h:4 * h + 4, 8:8 + s1],
                        a_send.at[c, h], a_recv.at[c, h], (0, -1, 0)) for h in range(2)] for c in range(GROUPS)]
    b_copies = [remote(raw[c].at[0:4, s1:s1 + 8], above[c], b_send.at[c], b_recv.at[c], (-1, 0, 0))
                for c in range(GROUPS)]
    for copy, step in zip(lane_copies, LANE_PEERS):
        @pl.when(exists(opposite(step)))
        def _():
            copy.start()

    @pl.when(exists((0, -1, 0)))
    def _():
        for c in range(GROUPS):
            for h in range(2):
                a_copies[c][h].start()

    edges = (
        ((-1, 0, 0), lambda c: box[c].at[0:3, 3:11]), ((1, 0, 0), lambda c: box[c].at[11:14, 3:11]),
        ((0, -1, 0), lambda c: box[c].at[3:11, 0:3]), ((0, 1, 0), lambda c: box[c].at[3:11, 11:14]),
        ((0, 0, -1), lambda c: arm_low[c]), ((0, 0, 1), lambda c: arm_high[c]))
    for step, view in edges:
        @pl.when(jnp.logical_not(exists(step)))
        def _():
            for c in range(GROUPS):
                ref = view(c)
                ref[...] = jnp.zeros(ref.shape, F32)

    loads[5].wait()
    loads[6].wait()
    for c in range(GROUPS):
        for k in range(12):
            q = k % 6
            source = advect if q < 3 else diffuse
            weight_f32[:, 8 * k:8 * k + 8] = source[q % 3, :, 8 * c:8 * c + 8] * (1.0 / 12.0)
        full = weight_f32[...]
        high = full.astype(BF16).astype(F32)
        weights[c] = jnp.concatenate([high, full - high], axis=0).astype(BF16)
    loads[3].wait()
    loads[4].wait()
    s0, s2 = shift[0], shift[2]

    for c in range(GROUPS):
        @pl.when(exists((0, 1, 0)))
        def _():
            a_copies[c][0].wait_recv()

        @pl.when(exists((-1, 0, 0)))
        def _():
            b_copies[c].start()

    for copy, step in zip(lane_copies, LANE_PEERS):
        @pl.when(exists(step))
        def _():
            copy.wait_recv()

    def arm(c, k, src, dst, step):
        return remote(src, dst, arm_send.at[c, k], arm_recv.at[c, k], step)

    def arms_of(c, h):
        xs = slice(3 + 4 * h, 7 + 4 * h)
        pair = slice(2 * h, 2 * h + 2)
        found = [
            (arm(c, 5 * h + 0, box[c].at[xs, 3:6], box[c].at[xs, 11:14], (0, -1, 0)), (0, -1, 0)),
            (arm(c, 5 * h + 1, box[c].at[xs, 8:11], box[c].at[xs, 0:3], (0, 1, 0)), (0, 1, 0)),
            (arm(c, 5 * h + 2, arm_out[c].at[pair], arm_high[c].at[pair], (0, 0, -1)), (0, 0, -1)),
            (arm(c, 5 * h + 3, arm_out[c].at[pair], arm_low[c].at[pair], (0, 0, 1)), (0, 0, 1))]
        if h == 0:
            found.append((arm(c, 4, box[c].at[3:6, 3:11], box[c].at[11:14, 3:11], (-1, 0, 0)), (-1, 0, 0)))
        else:
            found.append((arm(c, 9, box[c].at[8:11, 3:11], box[c].at[0:3, 3:11], (1, 0, 0)), (1, 0, 0)))
        return found

    arms = [[arms_of(c, h) for h in range(2)] for c in range(GROUPS)]

    def build(c, h):
        for pair in range(2):
            packed = zero
            for x2 in range(2):
                x = 4 * h + 2 * pair + x2
                parent_tiles = jnp.swapaxes(parent_v[8 * c:8 * c + 8, x], 0, 1)
                old = x + s0
                if h == 0:
                    part, at_lane = 0, 4 * (3 * old + c)
                else:
                    here = old < NX
                    part = jnp.where(here, 0, 1)
                    at_lane = 4 * (3 * jnp.where(here, old, old - NX) + c)
                    own_at, above_at = jnp.minimum(old, NX - 1), jnp.maximum(old - NX, 0)
                in_x = gx * NX + old < sizes[0] * NX
                back = lax.rem(2 * NZ - s2 - at_lane, NZ)
                for y in range(NY):
                    if h == 0:
                        own = raw[c][old, y + s1]
                    else:
                        own = jnp.where(here, raw[c][own_at, y + s1], above[c][above_at, y])
                    tile = jnp.where(lane < NZ - s2, pltpu.roll(own, NZ - s2, 1),
                                     pltpu.roll(lanes_in[part, y + s1], back, 1))
                    inside = in_x & (gy * NY + y + s1 < sizes[1] * NY)
                    limit = jnp.where(inside, sizes[2] * NZ - gz * NZ - s2, 0)
                    tile = jnp.where(lane < limit, tile, parent_tiles[y])
                    box[c][3 + x, 3 + y] = tile
                    at = 8 * x2 + y
                    packed = jnp.where(eight == at, pltpu.roll(tile, (8 * at + 4) % NZ, 1), packed)
            arm_out[c][2 * h + pair] = packed
        for copy, step in arms[c][h]:
            @pl.when(exists(step))
            def _():
                copy.start()

    for c in range(GROUPS):
        @pl.when(exists((0, 1, 0)))
        def _():
            a_copies[c][1].wait_recv()
        build(c, 0)

    for c in range(GROUPS):
        @pl.when(exists((1, 0, 0)))
        def _():
            b_copies[c].wait_recv()
        build(c, 1)

    def line(m3, m2, m1, u0, p1, p2, p3):
        d1, d2 = p1 - m1, p2 - m2
        t1, t2, t3 = p1 + m1, p2 + m2, p3 + m3
        return 8.0 * d1 - d2, 16.0 * t1 - t2 - 30.0 * u0, t3 - 6.0 * t2 + 15.0 * t1

    def work_one(c, x, h, pair, x2, slot):
        column = [box[c][3 + x, y] for y in range(14)]
        ends_pack = jnp.where(lane % 8 < 4, arm_low[c][2 * h + pair], arm_high[c][2 * h + pair])
        smooths = []
        for y in range(NY):
            at = 8 * x2 + y
            u0 = column[3 + y]
            ends = pltpu.roll(ends_pack, (2 * NZ - 8 * at - 4) % NZ, 1)
            before = [pltpu.roll(jnp.where(lane >= NZ - o, ends, u0), o, 1) for o in (3, 2, 1)]
            after = [pltpu.roll(jnp.where(lane < o, ends, u0), NZ - o, 1) for o in (1, 2, 3)]
            fz, sz, qz = line(*before, u0, *after)
            fy, sy, qy = line(*column[y:y + 7])
            fx, sx, qx = line(*[box[c][x + o, 3 + y] for o in range(3)], u0,
                              *[box[c][x + o, 3 + y] for o in range(4, 7)])
            smooths.append((qx + qy + qz - 60.0 * u0) * (1.0 / 64.0))
            full = jnp.concatenate([fx, fy, fz, sx, sy, sz], axis=0)
            top = full.astype(BF16)
            mixed[slot, 0:48, 128 * y:128 * y + 128] = top
            mixed[slot, 48:96, 128 * y:128 * y + 128] = (full - top.astype(F32)).astype(BF16)
        product = jnp.dot(weights[c], mixed[slot], preferred_element_type=F32)
        product = product[0:24] + product[24:48]
        if c > 0:
            product = acc[x] + product
        if c < GROUPS - 1:
            for y in range(NY):
                slope_v[8 * c + y, x] = smooths[y]
            acc[x] = product
            return
        factors = [1.0 + 0.25 * jnp.tanh(box[0][3 + x, 3 + y][0:1]) for y in range(NY)]
        for g in range(GROUPS):
            slopes, values = [], []
            for y in range(NY):
                smooth = smooths[y] if g == c else slope_v[8 * g + y, x]
                slope = factors[y] * product[8 * g:8 * g + 8, 128 * y:128 * y + 128] + smooth
                slopes.append(slope)
                values.append(box[g][3 + x, 3 + y] + 0.125 * slope)
            slope_v[8 * g:8 * g + 8, x] = jnp.swapaxes(jnp.stack(slopes), 0, 1)
            value_v[8 * g:8 * g + 8, x] = jnp.swapaxes(jnp.stack(values), 0, 1)

    def work(c, h):
        def body(pair, carry):
            for x2 in range(2):
                work_one(c, 4 * h + 2 * pair + x2, h, pair, x2, x2)
            return carry
        lax.fori_loop(0, 2, body, 0)

    stores = [[pltpu.make_async_copy(ref.at[:, 4 * h:4 * h + 4], hbm.at[:, 4 * h:4 * h + 4], store_sem.at[k, h])
               for k, (ref, hbm) in enumerate(((slope_v, slope_hbm), (value_v, value_hbm)))] for h in range(2)]

    def wait_arms(c, which):
        for h, k in which:
            copy, step = arms[c][h][k]

            @pl.when(exists(opposite(step)))
            def _():
                copy.wait_recv()

    for c in range(GROUPS):
        wait_arms(c, [(0, 0), (0, 1), (0, 2), (0, 3), (1, 4)])
        work(c, 0)
    for store in stores[0]:
        store.start()

    for c in range(GROUPS):
        wait_arms(c, [(1, 0), (1, 1), (1, 2), (1, 3), (0, 4)])
        work(c, 1)
    for store in stores[1]:
        store.start()

    for copy, step in zip(lane_copies, LANE_PEERS):
        @pl.when(exists(opposite(step)))
        def _():
            copy.wait_send()

    @pl.when(exists((0, -1, 0)))
    def _():
        for c in range(GROUPS):
            for h in range(2):
                a_copies[c][h].wait_send()

    @pl.when(exists((-1, 0, 0)))
    def _():
        for c in range(GROUPS):
            b_copies[c].wait_send()
    for c in range(GROUPS):
        for h in range(2):
            for copy, step in arms[c][h]:
                @pl.when(exists(step))
                def _():
                    copy.wait_send()
    for h in range(2):
        for store in stores[h]:
            store.wait()


def section(s1, fields_now, parent, advect, diffuse, box_shift):
    shape = jax.ShapeDtypeStruct(fields_now.shape, F32)
    whole = pltpu.VMEM(fields_now.shape, F32)
    packed = pltpu.VMEM((4, 8, NZ), F32)
    dma = pltpu.SemaphoreType.DMA
    scratch = [
        pltpu.SMEM((3,), jnp.int32), pltpu.VMEM(advect.shape, F32), pltpu.VMEM(diffuse.shape, F32),
        whole, whole, whole, whole, pltpu.VMEM((NX, 24, NY * NZ), F32),
        pltpu.VMEM((2, 96, NY * NZ), BF16), pltpu.VMEM((GROUPS, 48, 96), BF16), pltpu.VMEM((24, 96), F32),
        pltpu.VMEM((NY, 8, NZ), F32), pltpu.VMEM((2, NY + s1, 8, NZ), F32),
        *[pltpu.VMEM((NX, NY + s1, 8, NZ), F32)] * GROUPS,
        *[pltpu.VMEM((4, NY, 8, NZ), F32)] * GROUPS,
        *[pltpu.VMEM((14, 14, 8, NZ), F32)] * GROUPS,
        *[packed] * (3 * GROUPS),
        dma((7,)), dma((2, 2)), dma((GROUPS, 2)), dma((GROUPS, 2)), dma((GROUPS,)), dma((GROUPS,)),
        dma((4,)), dma((4,)), dma((GROUPS, 10)), dma((GROUPS, 10)),
    ]
    hbm = pl.BlockSpec(memory_space=pl.ANY)
    return pl.pallas_call(
        functools.partial(kernel, s1),
        out_shape=(shape, shape),
        in_specs=[hbm] * 5,
        out_specs=(hbm, hbm),
        scratch_shapes=scratch,
        compiler_params=pltpu.CompilerParams(collective_id=s1, has_side_effects=True),
        name=f"section{s1}",
    )(box_shift, fields_now, parent, advect, diffuse)


def local(fields_now, parent, advect, diffuse, box_shift):
    branches = [functools.partial(section, s1) for s1 in range(1, 5)]
    return lax.switch(box_shift[1] - 1, branches, fields_now, parent, advect, diffuse, box_shift)


def solution(mesh):
    return jax.shard_map(
        local,
        mesh=mesh,
        in_specs=(P(None, "gx", "gy", "gz"), P(None, "gx", "gy", "gz"), P(), P(), P()),
        out_specs=(P(None, "gx", "gy", "gz"), P(None, "gx", "gy", "gz")),
        check_vma=False,
    )
```

```python
import jax
import jax.numpy as jnp
from jax import lax
from jax.experimental import pallas as pl
from jax.experimental.pallas import tpu as pltpu
from jax.sharding import PartitionSpec as P

MESH = pl.DeviceIdType.MESH
F32, BF16 = jnp.float32, jnp.bfloat16
GROUPS = 3
NX, NY, NZ = 8, 8, 128
REACH = 4
AXES = ("gx", "gy", "gz")
FACES = ((0, 0, 1), (0, 1, 0), (1, 0, 0))


def kernel(shift_hbm, now_hbm, parent_hbm, advect_hbm, diffuse_hbm, slope_v, value_v, *scratch):
    scratch = list(scratch)

    def take(count):
        got = scratch[:count]
        del scratch[:count]
        return got

    shift, advect, diffuse, now_v, parent_v, acc = take(6)
    mixed, mixed_y, weights_xz, weights_y, weight_f32, lanes_out, lanes_in, lanes = take(8)
    raw = [take(2) for _ in range(GROUPS)]
    moved, above, box = take(GROUPS), take(GROUPS), take(GROUPS)
    arm_out, arm_low, arm_high = take(GROUPS), take(GROUPS), take(GROUPS)
    load_sem, a_send, a_recv, b_send, b_recv, z_send, z_recv, arm_send, arm_recv = take(10)

    place = [lax.axis_index(axis) for axis in AXES]
    sizes = [lax.axis_size(axis) for axis in AXES]
    gx, gy, gz = place

    def exists(step):
        found = None
        for at, size, by in zip(place, sizes, step):
            if by:
                inside = (at < size - 1) if by > 0 else (at > 0)
                found = inside if found is None else found & inside
        return found

    def peer(step):
        return {axis: at + by for axis, at, by in zip(AXES, place, step) if by}

    def remote(src, dst, send, recv, step):
        return pltpu.make_async_remote_copy(
            src_ref=src, dst_ref=dst, send_sem=send, recv_sem=recv, device_id=peer(step), device_id_type=MESH)

    def opposite(step):
        return tuple(-by for by in step)

    barrier = pltpu.get_barrier_semaphore()
    steps = []
    for step in FACES + ((0, 1, 1),):
        steps += [step, opposite(step)]
    for step in steps:
        @pl.when(exists(step))
        def _():
            pl.semaphore_signal(barrier, inc=1, device_id=peer(step), device_id_type=MESH)

    loads = [pltpu.make_async_copy(now_hbm.at[pl.ds(8 * c, 8)], now_v.at[pl.ds(8 * c, 8)], load_sem.at[c])
             for c in range(GROUPS)]
    loads.append(pltpu.make_async_copy(shift_hbm, shift, load_sem.at[3]))
    loads.append(pltpu.make_async_copy(parent_hbm, parent_v, load_sem.at[4]))
    loads.append(pltpu.make_async_copy(advect_hbm, advect, load_sem.at[5]))
    loads.append(pltpu.make_async_copy(diffuse_hbm, diffuse, load_sem.at[6]))
    for load in loads:
        load.start()

    lane = lax.broadcasted_iota(jnp.int32, (8, NZ), 1)
    four, eight = lane // 4, lane // 8
    zero = jnp.zeros((8, NZ), F32)

    def turn(c, packed):
        loads[c].wait()
        for x in range(NX):
            tiles = jnp.swapaxes(now_v[8 * c:8 * c + 8, x], 0, 1)
            raw[c][x // 4][x % 4, 0:8] = tiles
            at = 3 * x + c
            packed = [jnp.where(four == at, pltpu.roll(tiles[y], 4 * at, 1), packed[y]) for y in range(NY)]
        return packed

    packed = turn(0, [zero] * NY)

    pl.semaphore_wait(barrier, sum(exists(step).astype(jnp.int32) for step in steps))

    lane_copies = [
        remote(lanes_out, lanes_in.at[0:8], z_send.at[0], z_recv.at[0], (0, 0, -1)),
        remote(lanes_out.at[0:REACH], lanes_in.at[8:8 + REACH], z_send.at[1], z_recv.at[1], (0, -1, -1)),
        remote(lanes.at[0], lanes.at[1], z_send.at[2], z_recv.at[2], (-1, 0, 0))]
    has_lanes = exists((0, 0, 1))
    lane_sent = [exists((0, 0, -1)), exists((0, -1, -1)), has_lanes & exists((-1, 0, 0))]
    lane_received = [has_lanes, exists((0, 1, 1)), has_lanes & exists((1, 0, 0))]
    a_copies = [[remote(raw[c][h].at[:, 0:REACH], raw[c][h].at[:, 8:8 + REACH],
                        a_send.at[c, h], a_recv.at[c, h], (0, -1, 0)) for h in range(2)] for c in range(GROUPS)]
    b_copies = [remote(moved[c].at[0:REACH], above[c], b_send.at[c], b_recv.at[c], (-1, 0, 0))
                for c in range(GROUPS)]
    def send_rows(c):
        @pl.when(exists((0, -1, 0)))
        def _():
            for h in range(2):
                a_copies[c][h].start()

    send_rows(0)
    for c in range(1, GROUPS):
        packed = turn(c, packed)
    for y in range(NY):
        lanes_out[y] = packed[y]
    for k in range(2):
        @pl.when(lane_sent[k])
        def _():
            lane_copies[k].start()
    for c in range(1, GROUPS):
        send_rows(c)

    edges = (
        ((-1, 0, 0), lambda c: box[c].at[0:3, 3:11]), ((1, 0, 0), lambda c: box[c].at[11:14, 3:11]),
        ((0, -1, 0), lambda c: box[c].at[3:11, 0:3]), ((0, 1, 0), lambda c: box[c].at[3:11, 11:14]),
        ((0, 0, -1), lambda c: arm_low[c]), ((0, 0, 1), lambda c: arm_high[c]))
    for step, view in edges:
        @pl.when(jnp.logical_not(exists(step)))
        def _():
            for c in range(GROUPS):
                ref = view(c)
                ref[...] = jnp.zeros(ref.shape, F32)

    loads[5].wait()
    loads[6].wait()
    for c in range(GROUPS):
        for k, q in enumerate((0, 2, 3, 5) * 2 + (1, 4) * 2):
            source, scale = (advect, 8.0 / 12.0) if q < 3 else (diffuse, 16.0 / 12.0)
            weight_f32[:, 8 * k:8 * k + 8] = source[q % 3, :, 8 * c:8 * c + 8] * scale
        full = weight_f32[...]
        high = full.astype(BF16).astype(F32)
        both = jnp.concatenate([high, full - high], axis=0).astype(BF16)
        weights_xz[c] = both[:, 0:64]
        weights_y[c] = both[:, 64:96]
    loads[3].wait()
    loads[4].wait()
    s0, s1, s2 = shift[0], shift[1], shift[2]

    def arm(c, k, src, dst, step):
        return remote(src, dst, arm_send.at[c, k], arm_recv.at[c, k], step)

    def arms_of(c, h):
        xs = slice(3 + 4 * h, 7 + 4 * h)
        pair = slice(2 * h, 2 * h + 2)
        found = [
            (arm(c, 5 * h + 0, box[c].at[xs, 3:6], box[c].at[xs, 11:14], (0, -1, 0)), (0, -1, 0)),
            (arm(c, 5 * h + 1, box[c].at[xs, 8:11], box[c].at[xs, 0:3], (0, 1, 0)), (0, 1, 0)),
            (arm(c, 5 * h + 2, arm_out[c].at[pair], arm_high[c].at[pair], (0, 0, -1)), (0, 0, -1)),
            (arm(c, 5 * h + 3, arm_out[c].at[pair], arm_low[c].at[pair], (0, 0, 1)), (0, 0, 1))]
        if h == 0:
            found.append((arm(c, 4, box[c].at[3:6, 3:11], box[c].at[11:14, 3:11], (-1, 0, 0)), (-1, 0, 0)))
        else:
            found.append((arm(c, 9, box[c].at[8:11, 3:11], box[c].at[0:3, 3:11], (1, 0, 0)), (1, 0, 0)))
        return found

    arms = [[arms_of(c, h) for h in range(2)] for c in range(GROUPS)]

    def send_arms(some):
        for copy, step in some:
            @pl.when(exists(step))
            def _():
                copy.start()

    def build(c, h):
        for pair in range(2):
            packed = zero
            for x2 in range(2):
                x = 4 * h + 2 * pair + x2
                parent_tiles = jnp.swapaxes(parent_v[8 * c:8 * c + 8, x], 0, 1)
                old = x + s0
                if h == 0:
                    part, at_lane = 0, 4 * (3 * old + c)
                else:
                    here = old < NX
                    part = jnp.where(here, 0, 1)
                    at_lane = 4 * (3 * jnp.where(here, old, old - NX) + c)
                    own_at, above_at = jnp.minimum(old, NX - 1), jnp.maximum(old - NX, 0)
                in_x = gx * NX + old < sizes[0] * NX
                back = lax.rem(2 * NZ - s2 - at_lane, NZ)
                for y in range(NY):
                    if h == 0:
                        own = moved[c][old, y]
                    else:
                        own = jnp.where(here, moved[c][own_at, y], above[c][above_at, y])
                    tile = jnp.where(lane < NZ - s2, pltpu.roll(own, NZ - s2, 1),
                                     pltpu.roll(lanes[part, y], back, 1))
                    inside = in_x & (gy * NY + y + s1 < sizes[1] * NY)
                    limit = jnp.where(inside, sizes[2] * NZ - gz * NZ - s2, 0)
                    tile = jnp.where(lane < limit, tile, parent_tiles[y])
                    box[c][3 + x, 3 + y] = tile
                    at = 8 * x2 + y
                    packed = jnp.where(eight == at, pltpu.roll(tile, (8 * at + 4) % NZ, 1), packed)
            arm_out[c][2 * h + pair] = packed
        send_arms(arms[c][h][2:4] + arms[c][h][0:2])

    def shift_y(c, h):
        for x in range(4):
            for y in range(NY):
                moved[c][4 * h + x, y] = raw[c][h][x, y + s1]

    def take_rows(c, h):
        @pl.when(exists((0, 1, 0)))
        def _():
            a_copies[c][h].wait_recv()
        shift_y(c, h)

    def send_layers(c):
        take_rows(c, 0)

        @pl.when(exists((-1, 0, 0)))
        def _():
            b_copies[c].start()

    send_layers(0)
    take_rows(0, 1)
    for k in range(2):
        @pl.when(lane_received[k])
        def _():
            lane_copies[k].wait_recv()
    for y in range(NY):
        lanes[0, y] = lanes_in[y + s1]

    @pl.when(lane_sent[2])
    def _():
        lane_copies[2].start()
    build(0, 0)
    for c in range(1, GROUPS):
        send_layers(c)
        take_rows(c, 1)
        build(c, 0)

    for c in range(GROUPS):
        send_arms(arms[c][0][4:])

    @pl.when(lane_received[2])
    def _():
        lane_copies[2].wait_recv()
    for c in range(GROUPS):
        @pl.when(exists((1, 0, 0)))
        def _():
            b_copies[c].wait_recv()
        build(c, 1)
        send_arms(arms[c][1][4:])

    def line(m3, m2, m1, middle, p1, p2, p3):
        t1, t2, t3 = p1 + m1, p2 + m2, p3 + m3
        first = (p1 - m1) - 0.125 * (p2 - m2)
        second = (t1 - 0.0625 * t2) - middle
        return first, second, t1, t2, t3

    def sixth(t1, t2, t3):
        return ((15.0 / 64.0) * t1 - (6.0 / 64.0) * t2) + (1.0 / 64.0) * t3

    def put(ref, slot, y, parts):
        full = jnp.concatenate(parts, axis=0)
        rows = full.shape[0]
        top = full.astype(BF16)
        ref[slot, 0:rows, 128 * y:128 * y + 128] = top
        ref[slot, rows:2 * rows, 128 * y:128 * y + 128] = (full - top.astype(F32)).astype(BF16)

    def mix(weights, ref, slot):
        product = jnp.dot(weights, ref[slot], preferred_element_type=F32)
        return product[0:24] + product[24:48]

    def along_xz(c, x, h, pair, x2, slot):
        ends_pack = jnp.where(lane % 8 < 4, arm_low[c][2 * h + pair], arm_high[c][2 * h + pair])
        for y in range(NY):
            at = 8 * x2 + y
            u0 = box[c][3 + x, 3 + y]
            ends = pltpu.roll(ends_pack, (2 * NZ - 8 * at - 4) % NZ, 1)
            before = [pltpu.roll(jnp.where(lane >= NZ - o, ends, u0), o, 1) for o in (3, 2, 1)]
            after = [pltpu.roll(jnp.where(lane < o, ends, u0), NZ - o, 1) for o in (1, 2, 3)]
            middle = 1.875 * u0
            fz, sz, *tz = line(*before, middle, *after)
            fx, sx, *tx = line(*[box[c][x + o, 3 + y] for o in range(3)], middle,
                               *[box[c][x + o, 3 + y] for o in range(4, 7)])
            slope_v[8 * c + y, x] = sixth(*[i + k for i, k in zip(tx, tz)]) - (60.0 / 64.0) * u0
            put(mixed, slot, y, [fx, fz, sx, sz])
        product = mix(weights_xz[c], mixed, slot)
        acc[x] = product if c == 0 else acc[x] + product

    def along_y(c, x, slot):
        column = [box[c][3 + x, y] for y in range(14)]
        smooths = []
        for y in range(NY):
            fy, sy, *ty = line(*column[y:y + 3], 1.875 * column[3 + y], *column[y + 4:y + 7])
            smooths.append(slope_v[8 * c + y, x] + sixth(*ty))
            put(mixed_y, slot, y, [fy, sy])
        product = acc[x] + mix(weights_y[c], mixed_y, slot)
        if c < GROUPS - 1:
            for y in range(NY):
                slope_v[8 * c + y, x] = smooths[y]
            acc[x] = product
            return
        factors = [1.0 + 0.25 * jnp.tanh(box[0][3 + x, 3 + y][0:1]) for y in range(NY)]
        for g in range(GROUPS):
            slopes, values = [], []
            for y in range(NY):
                smooth = smooths[y] if g == c else slope_v[8 * g + y, x]
                slope = factors[y] * product[8 * g:8 * g + 8, 128 * y:128 * y + 128] + smooth
                slopes.append(slope)
                values.append(box[g][3 + x, 3 + y] + 0.125 * slope)
            slope_v[8 * g:8 * g + 8, x] = jnp.swapaxes(jnp.stack(slopes), 0, 1)
            value_v[8 * g:8 * g + 8, x] = jnp.swapaxes(jnp.stack(values), 0, 1)

    def wait_arms(c, which):
        for h, k in which:
            copy, step = arms[c][h][k]

            @pl.when(exists(opposite(step)))
            def _():
                copy.wait_recv()

    needs_xz = ([(0, 2), (0, 3), (1, 4)], [(1, 2), (1, 3), (0, 4)])
    for axis, c, h in (("xz", 0, 0), ("xz", 1, 0), ("xz", 2, 0), ("y", 0, 0), ("y", 1, 0), ("xz", 0, 1), ("xz", 1, 1),
                       ("xz", 2, 1), ("y", 2, 0), ("y", 0, 1), ("y", 1, 1), ("y", 2, 1)):
        wait_arms(c, needs_xz[h] if axis == "xz" else [(h, 0), (h, 1)])
        for x4 in range(4):
            if axis == "xz":
                along_xz(c, 4 * h + x4, h, x4 // 2, x4 % 2, x4)
            else:
                along_y(c, 4 * h + x4, x4)

    for copy, sent in zip(lane_copies, lane_sent):
        @pl.when(sent)
        def _():
            copy.wait_send()

    @pl.when(exists((0, -1, 0)))
    def _():
        for c in range(GROUPS):
            for h in range(2):
                a_copies[c][h].wait_send()

    @pl.when(exists((-1, 0, 0)))
    def _():
        for c in range(GROUPS):
            b_copies[c].wait_send()
    for c in range(GROUPS):
        for h in range(2):
            for copy, step in arms[c][h]:
                @pl.when(exists(step))
                def _():
                    copy.wait_send()


def section(fields_now, parent, advect, diffuse, box_shift):
    whole = held = pltpu.VMEM(fields_now.shape, F32)
    packed = pltpu.VMEM((4, 8, NZ), F32)
    dma = pltpu.SemaphoreType.DMA
    scratch = [
        pltpu.SMEM((3,), jnp.int32), pltpu.VMEM(advect.shape, F32), pltpu.VMEM(diffuse.shape, F32),
        whole, whole, pltpu.VMEM((NX, 24, NY * NZ), F32),
        pltpu.VMEM((4, 64, NY * NZ), BF16), pltpu.VMEM((4, 32, NY * NZ), BF16),
        pltpu.VMEM((GROUPS, 48, 64), BF16), pltpu.VMEM((GROUPS, 48, 32), BF16), pltpu.VMEM((24, 96), F32),
        pltpu.VMEM((NY, 8, NZ), F32), pltpu.VMEM((NY + REACH, 8, NZ), F32), pltpu.VMEM((2, NY, 8, NZ), F32),
        *[pltpu.VMEM((4, NY + REACH, 8, NZ), F32)] * (2 * GROUPS),
        *[pltpu.VMEM((NX, NY, 8, NZ), F32)] * GROUPS,
        *[pltpu.VMEM((REACH, NY, 8, NZ), F32)] * GROUPS,
        *[pltpu.VMEM((14, 14, 8, NZ), F32)] * GROUPS,
        *[packed] * (3 * GROUPS),
        dma((7,)), dma((GROUPS, 2)), dma((GROUPS, 2)), dma((GROUPS,)), dma((GROUPS,)),
        dma((3,)), dma((3,)), dma((GROUPS, 10)), dma((GROUPS, 10)),
    ]
    hbm = pl.BlockSpec(memory_space=pl.ANY)
    return pl.pallas_call(
        kernel,
        out_shape=(held, held),
        in_specs=[pl.BlockSpec(memory_space=pltpu.HBM)] + [hbm] * 4,
        out_specs=(pl.BlockSpec(memory_space=pltpu.VMEM),) * 2,
        scratch_shapes=scratch,
        compiler_params=pltpu.CompilerParams(collective_id=0, has_side_effects=True),
        name="section",
    )(box_shift, fields_now, parent, advect, diffuse)


def out_kernel(slope, value, slope_hbm, value_hbm, sem):
    copies = [pltpu.make_async_copy(slope, slope_hbm, sem.at[0]), pltpu.make_async_copy(value, value_hbm, sem.at[1])]
    for copy in copies:
        copy.start()
    for copy in copies:
        copy.wait()


def hand_out(slope, value):
    shape = jax.ShapeDtypeStruct(slope.shape, F32)
    hbm = pl.BlockSpec(memory_space=pl.ANY)
    slope, value = [pltpu.with_memory_space_constraint(a, pltpu.VMEM) for a in (slope, value)]
    return pl.pallas_call(
        out_kernel, out_shape=(shape, shape), in_specs=[hbm] * 2, out_specs=(hbm, hbm),
        scratch_shapes=[pltpu.SemaphoreType.DMA((2,))], name="out")(slope, value)


def local(fields_now, parent, advect, diffuse, box_shift):
    return hand_out(*section(fields_now, parent, advect, diffuse, box_shift))


def solution(mesh):
    return jax.shard_map(
        local,
        mesh=mesh,
        in_specs=(P(None, "gx", "gy", "gz"), P(None, "gx", "gy", "gz"), P(), P(), P()),
        out_specs=(P(None, "gx", "gy", "gz"), P(None, "gx", "gy", "gz")),
        check_vma=False,
    )
```

```python
import jax
import jax.numpy as jnp
from jax import lax
from jax.experimental import pallas as pl
from jax.experimental.pallas import tpu as pltpu
from jax.sharding import PartitionSpec as P

MESH = pl.DeviceIdType.MESH
F32, BF16 = jnp.float32, jnp.bfloat16
GROUPS = 3
NX, NY, NZ = 8, 8, 128
REACH = 4
AXES = ("gx", "gy", "gz")
FACES = ((0, 0, 1), (0, 1, 0), (1, 0, 0))


def kernel(shift_hbm, now_hbm, parent_hbm, advect_hbm, diffuse_hbm, slope_v, value_v, *scratch):
    scratch = list(scratch)

    def take(count):
        got = scratch[:count]
        del scratch[:count]
        return got

    shift, advect, diffuse, now_v, parent_v, acc = take(6)
    mixed, mixed_y, weights_xz, weights_y, weight_f32, lanes_out, lanes_in, lanes = take(8)
    raw = [take(2) for _ in range(GROUPS)]
    moved, above, box = take(GROUPS), take(GROUPS), take(GROUPS)
    arm_out, arm_low, arm_high = take(GROUPS), take(GROUPS), take(GROUPS)
    load_sem, a_send, a_recv, b_send, b_recv, z_send, z_recv, arm_send, arm_recv = take(10)

    place = [lax.axis_index(axis) for axis in AXES]
    sizes = [lax.axis_size(axis) for axis in AXES]
    gx, gy, gz = place

    def exists(step):
        found = None
        for at, size, by in zip(place, sizes, step):
            if by:
                inside = (at < size - 1) if by > 0 else (at > 0)
                found = inside if found is None else found & inside
        return found

    def peer(step):
        return {axis: at + by for axis, at, by in zip(AXES, place, step) if by}

    def remote(src, dst, send, recv, step):
        return pltpu.make_async_remote_copy(
            src_ref=src, dst_ref=dst, send_sem=send, recv_sem=recv, device_id=peer(step), device_id_type=MESH)

    def opposite(step):
        return tuple(-by for by in step)

    barrier = pltpu.get_barrier_semaphore()
    steps = []
    for step in FACES + ((0, 1, 1),):
        steps += [step, opposite(step)]
    for step in steps:
        @pl.when(exists(step))
        def _():
            pl.semaphore_signal(barrier, inc=1, device_id=peer(step), device_id_type=MESH)

    loads = [pltpu.make_async_copy(now_hbm.at[pl.ds(8 * c, 8)], now_v.at[pl.ds(8 * c, 8)], load_sem.at[c])
             for c in range(GROUPS)]
    loads.append(pltpu.make_async_copy(shift_hbm, shift, load_sem.at[3]))
    loads.append(pltpu.make_async_copy(parent_hbm, parent_v, load_sem.at[4]))
    loads.append(pltpu.make_async_copy(advect_hbm, advect, load_sem.at[5]))
    loads.append(pltpu.make_async_copy(diffuse_hbm, diffuse, load_sem.at[6]))
    for load in loads:
        load.start()

    lane = lax.broadcasted_iota(jnp.int32, (8, NZ), 1)
    four, eight = lane // 4, lane // 8
    zero = jnp.zeros((8, NZ), F32)

    def turn(c, packed):
        loads[c].wait()
        for x in range(NX):
            tiles = jnp.swapaxes(now_v[8 * c:8 * c + 8, x], 0, 1)
            raw[c][x // 4][x % 4, 0:8] = tiles
            at = 3 * x + c
            packed = [jnp.where(four == at, pltpu.roll(tiles[y], 4 * at, 1), packed[y]) for y in range(NY)]
        return packed

    packed = [zero] * NY
    for c in range(GROUPS):
        packed = turn(c, packed)
    for y in range(NY):
        lanes_out[y] = packed[y]

    pl.semaphore_wait(barrier, sum(exists(step).astype(jnp.int32) for step in steps))

    lane_copies = [
        remote(lanes_out, lanes_in.at[0:8], z_send.at[0], z_recv.at[0], (0, 0, -1)),
        remote(lanes_out.at[0:REACH], lanes_in.at[8:8 + REACH], z_send.at[1], z_recv.at[1], (0, -1, -1)),
        remote(lanes.at[0], lanes.at[1], z_send.at[2], z_recv.at[2], (-1, 0, 0))]
    has_lanes = exists((0, 0, 1))
    lane_sent = [exists((0, 0, -1)), exists((0, -1, -1)), has_lanes & exists((-1, 0, 0))]
    lane_received = [has_lanes, exists((0, 1, 1)), has_lanes & exists((1, 0, 0))]
    a_copies = [[remote(raw[c][h].at[:, 0:REACH], raw[c][h].at[:, 8:8 + REACH],
                        a_send.at[c, h], a_recv.at[c, h], (0, -1, 0)) for h in range(2)] for c in range(GROUPS)]
    b_copies = [remote(moved[c].at[0:REACH], above[c], b_send.at[c], b_recv.at[c], (-1, 0, 0))
                for c in range(GROUPS)]
    for k in range(2):
        @pl.when(lane_sent[k])
        def _():
            lane_copies[k].start()
    @pl.when(exists((0, -1, 0)))
    def _():
        for h in range(2):
            for c in range(GROUPS):
                a_copies[c][h].start()

    edges = (
        ((-1, 0, 0), lambda c: box[c].at[0:3, 3:11]), ((1, 0, 0), lambda c: box[c].at[11:14, 3:11]),
        ((0, -1, 0), lambda c: box[c].at[3:11, 0:3]), ((0, 1, 0), lambda c: box[c].at[3:11, 11:14]),
        ((0, 0, -1), lambda c: arm_low[c]), ((0, 0, 1), lambda c: arm_high[c]))
    for step, view in edges:
        @pl.when(jnp.logical_not(exists(step)))
        def _():
            for c in range(GROUPS):
                ref = view(c)
                ref[...] = jnp.zeros(ref.shape, F32)

    loads[5].wait()
    loads[6].wait()
    for c in range(GROUPS):
        for k, q in enumerate((0, 2, 3, 5) * 2 + (1, 4) * 2):
            source, scale = (advect, 8.0 / 12.0) if q < 3 else (diffuse, 16.0 / 12.0)
            weight_f32[:, 8 * k:8 * k + 8] = source[q % 3, :, 8 * c:8 * c + 8] * scale
        full = weight_f32[...]
        high = full.astype(BF16).astype(F32)
        both = jnp.concatenate([high, full - high], axis=0).astype(BF16)
        weights_xz[c] = both[:, 0:64]
        weights_y[c] = both[:, 64:96]
    loads[3].wait()
    loads[4].wait()
    s0, s1, s2 = shift[0], shift[1], shift[2]

    def arm(c, k, src, dst, step):
        return remote(src, dst, arm_send.at[c, k], arm_recv.at[c, k], step)

    def arms_of(c, h):
        xs = slice(3 + 4 * h, 7 + 4 * h)
        pair = slice(2 * h, 2 * h + 2)
        found = [
            (arm(c, 5 * h + 0, box[c].at[xs, 3:6], box[c].at[xs, 11:14], (0, -1, 0)), (0, -1, 0)),
            (arm(c, 5 * h + 1, box[c].at[xs, 8:11], box[c].at[xs, 0:3], (0, 1, 0)), (0, 1, 0)),
            (arm(c, 5 * h + 2, arm_out[c].at[pair], arm_high[c].at[pair], (0, 0, -1)), (0, 0, -1)),
            (arm(c, 5 * h + 3, arm_out[c].at[pair], arm_low[c].at[pair], (0, 0, 1)), (0, 0, 1))]
        if h == 0:
            found.append((arm(c, 4, box[c].at[3:6, 3:11], box[c].at[11:14, 3:11], (-1, 0, 0)), (-1, 0, 0)))
        else:
            found.append((arm(c, 9, box[c].at[8:11, 3:11], box[c].at[0:3, 3:11], (1, 0, 0)), (1, 0, 0)))
        return found

    arms = [[arms_of(c, h) for h in range(2)] for c in range(GROUPS)]

    def send_arms(some):
        for copy, step in some:
            @pl.when(exists(step))
            def _():
                copy.start()

    def build(c, h):
        for pair in range(2):
            packed = zero
            for x2 in range(2):
                x = 4 * h + 2 * pair + x2
                parent_tiles = jnp.swapaxes(parent_v[8 * c:8 * c + 8, x], 0, 1)
                old = x + s0
                if h == 0:
                    part, at_lane = 0, 4 * (3 * old + c)
                else:
                    here = old < NX
                    part = jnp.where(here, 0, 1)
                    at_lane = 4 * (3 * jnp.where(here, old, old - NX) + c)
                    own_at, above_at = jnp.minimum(old, NX - 1), jnp.maximum(old - NX, 0)
                in_x = gx * NX + old < sizes[0] * NX
                back = lax.rem(2 * NZ - s2 - at_lane, NZ)
                for y in range(NY):
                    if h == 0:
                        own = moved[c][old, y]
                    else:
                        own = jnp.where(here, moved[c][own_at, y], above[c][above_at, y])
                    tile = jnp.where(lane < NZ - s2, pltpu.roll(own, NZ - s2, 1),
                                     pltpu.roll(lanes[part, y], back, 1))
                    inside = in_x & (gy * NY + y + s1 < sizes[1] * NY)
                    limit = jnp.where(inside, sizes[2] * NZ - gz * NZ - s2, 0)
                    tile = jnp.where(lane < limit, tile, parent_tiles[y])
                    box[c][3 + x, 3 + y] = tile
                    at = 8 * x2 + y
                    packed = jnp.where(eight == at, pltpu.roll(tile, (8 * at + 4) % NZ, 1), packed)
            arm_out[c][2 * h + pair] = packed
        send_arms(arms[c][h][2:4] + arms[c][h][0:2])

    def shift_y(c, h):
        for x in range(4):
            for y in range(NY):
                moved[c][4 * h + x, y] = raw[c][h][x, y + s1]

    def take_rows(c, h):
        @pl.when(exists((0, 1, 0)))
        def _():
            a_copies[c][h].wait_recv()
        shift_y(c, h)

    def send_layers(c):
        take_rows(c, 0)

        @pl.when(exists((-1, 0, 0)))
        def _():
            b_copies[c].start()

    for c in range(GROUPS):
        send_layers(c)
    for k in range(2):
        @pl.when(lane_received[k])
        def _():
            lane_copies[k].wait_recv()
    for y in range(NY):
        lanes[0, y] = lanes_in[y + s1]

    @pl.when(lane_sent[2])
    def _():
        lane_copies[2].start()
    for c in range(GROUPS):
        take_rows(c, 1)
        build(c, 0)

    for c in range(GROUPS):
        send_arms(arms[c][0][4:])

    @pl.when(lane_received[2])
    def _():
        lane_copies[2].wait_recv()
    for c in range(GROUPS):
        @pl.when(exists((1, 0, 0)))
        def _():
            b_copies[c].wait_recv()
        build(c, 1)
        send_arms(arms[c][1][4:])

    def line(m3, m2, m1, middle, p1, p2, p3):
        t1, t2, t3 = p1 + m1, p2 + m2, p3 + m3
        first = (p1 - m1) - 0.125 * (p2 - m2)
        second = (t1 - 0.0625 * t2) - middle
        return first, second, t1, t2, t3

    def sixth(t1, t2, t3):
        return ((15.0 / 64.0) * t1 - (6.0 / 64.0) * t2) + (1.0 / 64.0) * t3

    def put(ref, slot, y, parts):
        full = jnp.concatenate(parts, axis=0)
        rows = full.shape[0]
        top = full.astype(BF16)
        ref[slot, 0:rows, 128 * y:128 * y + 128] = top
        ref[slot, rows:2 * rows, 128 * y:128 * y + 128] = (full - top.astype(F32)).astype(BF16)

    def mix(weights, ref, slot):
        product = jnp.dot(weights, ref[slot], preferred_element_type=F32)
        return product[0:24] + product[24:48]

    def along_xz(c, x, h, pair, x2, slot):
        ends_pack = jnp.where(lane % 8 < 4, arm_low[c][2 * h + pair], arm_high[c][2 * h + pair])
        for y in range(NY):
            at = 8 * x2 + y
            u0 = box[c][3 + x, 3 + y]
            ends = pltpu.roll(ends_pack, (2 * NZ - 8 * at - 4) % NZ, 1)
            before = [pltpu.roll(jnp.where(lane >= NZ - o, ends, u0), o, 1) for o in (3, 2, 1)]
            after = [pltpu.roll(jnp.where(lane < o, ends, u0), NZ - o, 1) for o in (1, 2, 3)]
            middle = 1.875 * u0
            fz, sz, *tz = line(*before, middle, *after)
            fx, sx, *tx = line(*[box[c][x + o, 3 + y] for o in range(3)], middle,
                               *[box[c][x + o, 3 + y] for o in range(4, 7)])
            slope_v[8 * c + y, x] = sixth(*[i + k for i, k in zip(tx, tz)]) - (60.0 / 64.0) * u0
            put(mixed, slot, y, [fx, fz, sx, sz])
        product = mix(weights_xz[c], mixed, slot)
        acc[x] = product if c == 0 else acc[x] + product

    def along_y(c, x, slot):
        column = [box[c][3 + x, y] for y in range(14)]
        smooths = []
        for y in range(NY):
            fy, sy, *ty = line(*column[y:y + 3], 1.875 * column[3 + y], *column[y + 4:y + 7])
            smooths.append(slope_v[8 * c + y, x] + sixth(*ty))
            put(mixed_y, slot, y, [fy, sy])
        product = acc[x] + mix(weights_y[c], mixed_y, slot)
        if c < GROUPS - 1:
            for y in range(NY):
                slope_v[8 * c + y, x] = smooths[y]
            acc[x] = product
            return
        factors = [1.0 + 0.25 * jnp.tanh(box[0][3 + x, 3 + y][0:1]) for y in range(NY)]
        for g in range(GROUPS):
            slopes, values = [], []
            for y in range(NY):
                smooth = smooths[y] if g == c else slope_v[8 * g + y, x]
                slope = factors[y] * product[8 * g:8 * g + 8, 128 * y:128 * y + 128] + smooth
                slopes.append(slope)
                values.append(box[g][3 + x, 3 + y] + 0.125 * slope)
            slope_v[8 * g:8 * g + 8, x] = jnp.swapaxes(jnp.stack(slopes), 0, 1)
            value_v[8 * g:8 * g + 8, x] = jnp.swapaxes(jnp.stack(values), 0, 1)

    def wait_arms(c, which):
        for h, k in which:
            copy, step = arms[c][h][k]

            @pl.when(exists(opposite(step)))
            def _():
                copy.wait_recv()

    needs_xz = ([(0, 2), (0, 3), (1, 4)], [(1, 2), (1, 3), (0, 4)])
    for axis, c, h in (("xz", 0, 0), ("xz", 1, 0), ("xz", 2, 0), ("y", 0, 0), ("y", 1, 0), ("xz", 0, 1), ("xz", 1, 1),
                       ("xz", 2, 1), ("y", 2, 0), ("y", 0, 1), ("y", 1, 1), ("y", 2, 1)):
        wait_arms(c, needs_xz[h] if axis == "xz" else [(h, 0), (h, 1)])
        for x4 in range(4):
            if axis == "xz":
                along_xz(c, 4 * h + x4, h, x4 // 2, x4 % 2, x4)
            else:
                along_y(c, 4 * h + x4, x4)

    for copy, sent in zip(lane_copies, lane_sent):
        @pl.when(sent)
        def _():
            copy.wait_send()

    @pl.when(exists((0, -1, 0)))
    def _():
        for c in range(GROUPS):
            for h in range(2):
                a_copies[c][h].wait_send()

    @pl.when(exists((-1, 0, 0)))
    def _():
        for c in range(GROUPS):
            b_copies[c].wait_send()
    for c in range(GROUPS):
        for h in range(2):
            for copy, step in arms[c][h]:
                @pl.when(exists(step))
                def _():
                    copy.wait_send()


def section(fields_now, parent, advect, diffuse, box_shift):
    whole = held = pltpu.VMEM(fields_now.shape, F32)
    packed = pltpu.VMEM((4, 8, NZ), F32)
    dma = pltpu.SemaphoreType.DMA
    scratch = [
        pltpu.SMEM((3,), jnp.int32), pltpu.VMEM(advect.shape, F32), pltpu.VMEM(diffuse.shape, F32),
        whole, whole, pltpu.VMEM((NX, 24, NY * NZ), F32),
        pltpu.VMEM((4, 64, NY * NZ), BF16), pltpu.VMEM((4, 32, NY * NZ), BF16),
        pltpu.VMEM((GROUPS, 48, 64), BF16), pltpu.VMEM((GROUPS, 48, 32), BF16), pltpu.VMEM((24, 96), F32),
        pltpu.VMEM((NY, 8, NZ), F32), pltpu.VMEM((NY + REACH, 8, NZ), F32), pltpu.VMEM((2, NY, 8, NZ), F32),
        *[pltpu.VMEM((4, NY + REACH, 8, NZ), F32)] * (2 * GROUPS),
        *[pltpu.VMEM((NX, NY, 8, NZ), F32)] * GROUPS,
        *[pltpu.VMEM((REACH, NY, 8, NZ), F32)] * GROUPS,
        *[pltpu.VMEM((14, 14, 8, NZ), F32)] * GROUPS,
        *[packed] * (3 * GROUPS),
        dma((7,)), dma((GROUPS, 2)), dma((GROUPS, 2)), dma((GROUPS,)), dma((GROUPS,)),
        dma((3,)), dma((3,)), dma((GROUPS, 10)), dma((GROUPS, 10)),
    ]
    hbm = pl.BlockSpec(memory_space=pl.ANY)
    return pl.pallas_call(
        kernel,
        out_shape=(held, held),
        in_specs=[pl.BlockSpec(memory_space=pltpu.HBM)] + [hbm] * 4,
        out_specs=(pl.BlockSpec(memory_space=pltpu.VMEM),) * 2,
        scratch_shapes=scratch,
        compiler_params=pltpu.CompilerParams(collective_id=0, has_side_effects=True),
        name="section",
    )(box_shift, fields_now, parent, advect, diffuse)


def out_kernel(slope, value, slope_hbm, value_hbm, sem):
    copies = [pltpu.make_async_copy(slope, slope_hbm, sem.at[0]), pltpu.make_async_copy(value, value_hbm, sem.at[1])]
    for copy in copies:
        copy.start()
    for copy in copies:
        copy.wait()


def hand_out(slope, value):
    shape = jax.ShapeDtypeStruct(slope.shape, F32)
    hbm = pl.BlockSpec(memory_space=pl.ANY)
    slope, value = [pltpu.with_memory_space_constraint(a, pltpu.VMEM) for a in (slope, value)]
    return pl.pallas_call(
        out_kernel, out_shape=(shape, shape), in_specs=[hbm] * 2, out_specs=(hbm, hbm),
        scratch_shapes=[pltpu.SemaphoreType.DMA((2,))], name="out")(slope, value)


def local(fields_now, parent, advect, diffuse, box_shift):
    return hand_out(*section(fields_now, parent, advect, diffuse, box_shift))


def solution(mesh):
    return jax.shard_map(
        local,
        mesh=mesh,
        in_specs=(P(None, "gx", "gy", "gz"), P(None, "gx", "gy", "gz"), P(), P(), P()),
        out_specs=(P(None, "gx", "gy", "gz"), P(None, "gx", "gy", "gz")),
        check_vma=False,
    )
```

```python
import jax
import jax.numpy as jnp
from jax import lax
from jax.experimental import pallas as pl
from jax.experimental.pallas import tpu as pltpu
from jax.sharding import PartitionSpec as P

MESH = pl.DeviceIdType.MESH
F32, BF16 = jnp.float32, jnp.bfloat16
GROUPS = 3
NX, NY, NZ = 8, 8, 128
REACH = 4
AXES = ("gx", "gy", "gz")
FACES = ((0, 0, 1), (0, 1, 0), (1, 0, 0))


def kernel(shift_hbm, now_hbm, parent_hbm, advect_hbm, diffuse_hbm, slope_v, value_v, *scratch):
    scratch = list(scratch)

    def take(count):
        got = scratch[:count]
        del scratch[:count]
        return got

    shift, advect, diffuse, now_v, parent_v, acc = take(6)
    mixed, mixed_y, weights_xz, weights_y, weight_f32, lanes_out, lanes_in, lanes = take(8)
    raw = [take(2) for _ in range(GROUPS)]
    moved, above, box = take(GROUPS), take(GROUPS), take(GROUPS)
    arm_out, arm_low, arm_high = take(GROUPS), take(GROUPS), take(GROUPS)
    load_sem, a_send, a_recv, b_send, b_recv, z_send, z_recv, arm_send, arm_recv = take(10)

    place = [lax.axis_index(axis) for axis in AXES]
    sizes = [lax.axis_size(axis) for axis in AXES]
    gx, gy, gz = place

    def exists(step):
        found = None
        for at, size, by in zip(place, sizes, step):
            if by:
                inside = (at < size - 1) if by > 0 else (at > 0)
                found = inside if found is None else found & inside
        return found

    def peer(step):
        return {axis: at + by for axis, at, by in zip(AXES, place, step) if by}

    def remote(src, dst, send, recv, step):
        return pltpu.make_async_remote_copy(
            src_ref=src, dst_ref=dst, send_sem=send, recv_sem=recv, device_id=peer(step), device_id_type=MESH)

    def opposite(step):
        return tuple(-by for by in step)

    barrier = pltpu.get_barrier_semaphore()
    steps = []
    for step in FACES + ((0, 1, 1),):
        steps += [step, opposite(step)]
    for step in steps:
        @pl.when(exists(step))
        def _():
            pl.semaphore_signal(barrier, inc=1, device_id=peer(step), device_id_type=MESH)

    loads = [pltpu.make_async_copy(now_hbm.at[pl.ds(8 * c, 8)], now_v.at[pl.ds(8 * c, 8)], load_sem.at[c])
             for c in range(GROUPS)]
    loads.append(pltpu.make_async_copy(shift_hbm, shift, load_sem.at[3]))
    loads.append(pltpu.make_async_copy(parent_hbm, parent_v, load_sem.at[4]))
    loads.append(pltpu.make_async_copy(advect_hbm, advect, load_sem.at[5]))
    loads.append(pltpu.make_async_copy(diffuse_hbm, diffuse, load_sem.at[6]))
    for load in loads:
        load.start()

    lane = lax.broadcasted_iota(jnp.int32, (8, NZ), 1)
    four = lane // 4
    zero = jnp.zeros((8, NZ), F32)

    def turn(c, packed):
        loads[c].wait()
        for x in range(NX):
            tiles = jnp.swapaxes(now_v[8 * c:8 * c + 8, x], 0, 1)
            raw[c][x // 4][x % 4, 0:8] = tiles
            at = 3 * x + c
            packed = [jnp.where(four == at, pltpu.roll(tiles[y], 4 * at, 1), packed[y]) for y in range(NY)]
        return packed

    packed = [zero] * NY
    for c in range(GROUPS):
        packed = turn(c, packed)
    for y in range(NY):
        lanes_out[y] = packed[y]

    pl.semaphore_wait(barrier, sum(exists(step).astype(jnp.int32) for step in steps))

    lane_copies = [
        remote(lanes_out, lanes_in.at[0:8], z_send.at[0], z_recv.at[0], (0, 0, -1)),
        remote(lanes_out.at[0:REACH], lanes_in.at[8:8 + REACH], z_send.at[1], z_recv.at[1], (0, -1, -1)),
        remote(lanes.at[0], lanes.at[1], z_send.at[2], z_recv.at[2], (-1, 0, 0))]
    has_lanes = exists((0, 0, 1))
    lane_sent = [exists((0, 0, -1)), exists((0, -1, -1)), has_lanes & exists((-1, 0, 0))]
    lane_received = [has_lanes, exists((0, 1, 1)), has_lanes & exists((1, 0, 0))]
    a_copies = [[remote(raw[c][h].at[:, 0:REACH], raw[c][h].at[:, 8:8 + REACH],
                        a_send.at[c, h], a_recv.at[c, h], (0, -1, 0)) for h in range(2)] for c in range(GROUPS)]
    b_copies = [remote(moved[c].at[0:REACH], above[c], b_send.at[c], b_recv.at[c], (-1, 0, 0))
                for c in range(GROUPS)]
    for k in range(2):
        @pl.when(lane_sent[k])
        def _():
            lane_copies[k].start()
    @pl.when(exists((0, -1, 0)))
    def _():
        for h in range(2):
            for c in range(GROUPS):
                a_copies[c][h].start()

    edges = (
        ((-1, 0, 0), lambda c: box[c].at[0:3, 3:11]), ((1, 0, 0), lambda c: box[c].at[11:14, 3:11]),
        ((0, -1, 0), lambda c: box[c].at[3:11, 0:3]), ((0, 1, 0), lambda c: box[c].at[3:11, 11:14]),
        ((0, 0, -1), lambda c: arm_low[c]), ((0, 0, 1), lambda c: arm_high[c]))
    for step, view in edges:
        @pl.when(jnp.logical_not(exists(step)))
        def _():
            for c in range(GROUPS):
                ref = view(c)
                ref[...] = jnp.zeros(ref.shape, F32)

    loads[5].wait()
    loads[6].wait()
    for c in range(GROUPS):
        for k, q in enumerate((0, 2, 3, 5) * 2 + (1, 4) * 2):
            source, scale = (advect, 8.0 / 12.0) if q < 3 else (diffuse, 16.0 / 12.0)
            weight_f32[:, 8 * k:8 * k + 8] = source[q % 3, :, 8 * c:8 * c + 8] * scale
        full = weight_f32[...]
        high = full.astype(BF16).astype(F32)
        both = jnp.concatenate([high, full - high], axis=0).astype(BF16)
        weights_xz[c] = both[:, 0:64]
        weights_y[c] = both[:, 64:96]
    loads[3].wait()
    loads[4].wait()
    s0, s1, s2 = shift[0], shift[1], shift[2]

    def arm(c, k, src, dst, step):
        return remote(src, dst, arm_send.at[c, k], arm_recv.at[c, k], step)

    def arms_of(c, h):
        xs = slice(3 + 4 * h, 7 + 4 * h)
        found = [
            (arm(c, 5 * h + 0, box[c].at[xs, 3:6], box[c].at[xs, 11:14], (0, -1, 0)), (0, -1, 0)),
            (arm(c, 5 * h + 1, box[c].at[xs, 8:11], box[c].at[xs, 0:3], (0, 1, 0)), (0, 1, 0)),
            (arm(c, 5 * h + 2, arm_out[c].at[h], arm_high[c].at[h], (0, 0, -1)), (0, 0, -1)),
            (arm(c, 5 * h + 3, arm_out[c].at[2 + h], arm_low[c].at[h], (0, 0, 1)), (0, 0, 1))]
        if h == 0:
            found.append((arm(c, 4, box[c].at[3:6, 3:11], box[c].at[11:14, 3:11], (-1, 0, 0)), (-1, 0, 0)))
        else:
            found.append((arm(c, 9, box[c].at[8:11, 3:11], box[c].at[0:3, 3:11], (1, 0, 0)), (1, 0, 0)))
        return found

    arms = [[arms_of(c, h) for h in range(2)] for c in range(GROUPS)]

    def send_arms(some):
        for copy, step in some:
            @pl.when(exists(step))
            def _():
                copy.start()

    def build(c, h):
        first_lanes = last_lanes = zero
        for pair in range(2):
            for x2 in range(2):
                x = 4 * h + 2 * pair + x2
                parent_tiles = jnp.swapaxes(parent_v[8 * c:8 * c + 8, x], 0, 1)
                old = x + s0
                if h == 0:
                    part, at_lane = 0, 4 * (3 * old + c)
                else:
                    here = old < NX
                    part = jnp.where(here, 0, 1)
                    at_lane = 4 * (3 * jnp.where(here, old, old - NX) + c)
                    own_at, above_at = jnp.minimum(old, NX - 1), jnp.maximum(old - NX, 0)
                in_x = gx * NX + old < sizes[0] * NX
                back = lax.rem(2 * NZ - s2 - at_lane, NZ)
                for y in range(NY):
                    if h == 0:
                        own = moved[c][old, y]
                    else:
                        own = jnp.where(here, moved[c][own_at, y], above[c][above_at, y])
                    tile = jnp.where(lane < NZ - s2, pltpu.roll(own, NZ - s2, 1),
                                     pltpu.roll(lanes[part, y], back, 1))
                    inside = in_x & (gy * NY + y + s1 < sizes[1] * NY)
                    limit = jnp.where(inside, sizes[2] * NZ - gz * NZ - s2, 0)
                    tile = jnp.where(lane < limit, tile, parent_tiles[y])
                    box[c][3 + x, 3 + y] = tile
                    at = 16 * pair + 8 * x2 + y
                    first_lanes = jnp.where(four == at, pltpu.roll(tile, 4 * at, 1), first_lanes)
                    last_lanes = jnp.where(four == at, pltpu.roll(tile, (4 * at + 4) % NZ, 1), last_lanes)
        arm_out[c][h] = first_lanes
        arm_out[c][2 + h] = last_lanes
        send_arms(arms[c][h][2:4] + arms[c][h][0:2])

    def shift_y(c, h):
        for x in range(4):
            for y in range(NY):
                moved[c][4 * h + x, y] = raw[c][h][x, y + s1]

    def take_rows(c, h):
        @pl.when(exists((0, 1, 0)))
        def _():
            a_copies[c][h].wait_recv()
        shift_y(c, h)

    def send_layers(c):
        take_rows(c, 0)

        @pl.when(exists((-1, 0, 0)))
        def _():
            b_copies[c].start()

    for c in range(GROUPS):
        send_layers(c)
    for k in range(2):
        @pl.when(lane_received[k])
        def _():
            lane_copies[k].wait_recv()
    for y in range(NY):
        lanes[0, y] = lanes_in[y + s1]

    @pl.when(lane_sent[2])
    def _():
        lane_copies[2].start()
    for c in range(GROUPS):
        take_rows(c, 1)
        build(c, 0)

    for c in range(GROUPS):
        send_arms(arms[c][0][4:])

    @pl.when(lane_received[2])
    def _():
        lane_copies[2].wait_recv()
    for c in range(GROUPS):
        @pl.when(exists((1, 0, 0)))
        def _():
            b_copies[c].wait_recv()
        build(c, 1)
        send_arms(arms[c][1][4:])

    def line(m3, m2, m1, middle, p1, p2, p3):
        t1, t2, t3 = p1 + m1, p2 + m2, p3 + m3
        first = (p1 - m1) - 0.125 * (p2 - m2)
        second = (t1 - 0.0625 * t2) - middle
        return first, second, t1, t2, t3

    def sixth(t1, t2, t3):
        return ((15.0 / 64.0) * t1 - (6.0 / 64.0) * t2) + (1.0 / 64.0) * t3

    def put(ref, slot, y, parts):
        full = jnp.concatenate(parts, axis=0)
        rows = full.shape[0]
        top = full.astype(BF16)
        ref[slot, 0:rows, 128 * y:128 * y + 128] = top
        ref[slot, rows:2 * rows, 128 * y:128 * y + 128] = (full - top.astype(F32)).astype(BF16)

    def mix(weights, ref, slot):
        product = jnp.dot(weights, ref[slot], preferred_element_type=F32)
        return product[0:24] + product[24:48]

    def along_xz(c, x, h, pair, x2, slot):
        low_pack, high_pack = arm_low[c][h], arm_high[c][h]
        for y in range(NY):
            at = 16 * pair + 8 * x2 + y
            u0 = box[c][3 + x, 3 + y]
            ends = jnp.where(lane < 64, pltpu.roll(high_pack, (NZ - 4 * at) % NZ, 1),
                             pltpu.roll(low_pack, (2 * NZ - 4 - 4 * at) % NZ, 1))
            before = [pltpu.roll(jnp.where(lane >= NZ - o, ends, u0), o, 1) for o in (3, 2, 1)]
            after = [pltpu.roll(jnp.where(lane < o, ends, u0), NZ - o, 1) for o in (1, 2, 3)]
            middle = 1.875 * u0
            fz, sz, *tz = line(*before, middle, *after)
            fx, sx, *tx = line(*[box[c][x + o, 3 + y] for o in range(3)], middle,
                               *[box[c][x + o, 3 + y] for o in range(4, 7)])
            slope_v[8 * c + y, x] = sixth(*[i + k for i, k in zip(tx, tz)]) - (60.0 / 64.0) * u0
            put(mixed, slot, y, [fx, fz, sx, sz])
        product = mix(weights_xz[c], mixed, slot)
        acc[x] = product if c == 0 else acc[x] + product

    def along_y(c, x, slot):
        column = [box[c][3 + x, y] for y in range(14)]
        smooths = []
        for y in range(NY):
            fy, sy, *ty = line(*column[y:y + 3], 1.875 * column[3 + y], *column[y + 4:y + 7])
            smooths.append(slope_v[8 * c + y, x] + sixth(*ty))
            put(mixed_y, slot, y, [fy, sy])
        product = acc[x] + mix(weights_y[c], mixed_y, slot)
        if c < GROUPS - 1:
            for y in range(NY):
                slope_v[8 * c + y, x] = smooths[y]
            acc[x] = product
            return
        factors = [1.0 + 0.25 * jnp.tanh(box[0][3 + x, 3 + y][0:1]) for y in range(NY)]
        for g in range(GROUPS):
            slopes, values = [], []
            for y in range(NY):
                smooth = smooths[y] if g == c else slope_v[8 * g + y, x]
                slope = factors[y] * product[8 * g:8 * g + 8, 128 * y:128 * y + 128] + smooth
                slopes.append(slope)
                values.append(box[g][3 + x, 3 + y] + 0.125 * slope)
            slope_v[8 * g:8 * g + 8, x] = jnp.swapaxes(jnp.stack(slopes), 0, 1)
            value_v[8 * g:8 * g + 8, x] = jnp.swapaxes(jnp.stack(values), 0, 1)

    def wait_arms(c, which):
        for h, k in which:
            copy, step = arms[c][h][k]

            @pl.when(exists(opposite(step)))
            def _():
                copy.wait_recv()

    needs_xz = ([(0, 2), (0, 3), (1, 4)], [(1, 2), (1, 3), (0, 4)])
    for axis, c, h in (("xz", 0, 0), ("xz", 1, 0), ("xz", 2, 0), ("y", 0, 0), ("y", 1, 0), ("xz", 0, 1), ("xz", 1, 1),
                       ("xz", 2, 1), ("y", 2, 0), ("y", 0, 1), ("y", 1, 1), ("y", 2, 1)):
        wait_arms(c, needs_xz[h] if axis == "xz" else [(h, 0), (h, 1)])
        for x4 in range(4):
            if axis == "xz":
                along_xz(c, 4 * h + x4, h, x4 // 2, x4 % 2, x4)
            else:
                along_y(c, 4 * h + x4, x4)

    for copy, sent in zip(lane_copies, lane_sent):
        @pl.when(sent)
        def _():
            copy.wait_send()

    @pl.when(exists((0, -1, 0)))
    def _():
        for c in range(GROUPS):
            for h in range(2):
                a_copies[c][h].wait_send()

    @pl.when(exists((-1, 0, 0)))
    def _():
        for c in range(GROUPS):
            b_copies[c].wait_send()
    for c in range(GROUPS):
        for h in range(2):
            for copy, step in arms[c][h]:
                @pl.when(exists(step))
                def _():
                    copy.wait_send()


def section(fields_now, parent, advect, diffuse, box_shift):
    whole = held = pltpu.VMEM(fields_now.shape, F32)
    packed = pltpu.VMEM((4, 8, NZ), F32)
    dma = pltpu.SemaphoreType.DMA
    scratch = [
        pltpu.SMEM((3,), jnp.int32), pltpu.VMEM(advect.shape, F32), pltpu.VMEM(diffuse.shape, F32),
        whole, whole, pltpu.VMEM((NX, 24, NY * NZ), F32),
        pltpu.VMEM((4, 64, NY * NZ), BF16), pltpu.VMEM((4, 32, NY * NZ), BF16),
        pltpu.VMEM((GROUPS, 48, 64), BF16), pltpu.VMEM((GROUPS, 48, 32), BF16), pltpu.VMEM((24, 96), F32),
        pltpu.VMEM((NY, 8, NZ), F32), pltpu.VMEM((NY + REACH, 8, NZ), F32), pltpu.VMEM((2, NY, 8, NZ), F32),
        *[pltpu.VMEM((4, NY + REACH, 8, NZ), F32)] * (2 * GROUPS),
        *[pltpu.VMEM((NX, NY, 8, NZ), F32)] * GROUPS,
        *[pltpu.VMEM((REACH, NY, 8, NZ), F32)] * GROUPS,
        *[pltpu.VMEM((14, 14, 8, NZ), F32)] * GROUPS,
        *[packed] * (3 * GROUPS),
        dma((7,)), dma((GROUPS, 2)), dma((GROUPS, 2)), dma((GROUPS,)), dma((GROUPS,)),
        dma((3,)), dma((3,)), dma((GROUPS, 10)), dma((GROUPS, 10)),
    ]
    hbm = pl.BlockSpec(memory_space=pl.ANY)
    return pl.pallas_call(
        kernel,
        out_shape=(held, held),
        in_specs=[pl.BlockSpec(memory_space=pltpu.HBM)] + [hbm] * 4,
        out_specs=(pl.BlockSpec(memory_space=pltpu.VMEM),) * 2,
        scratch_shapes=scratch,
        compiler_params=pltpu.CompilerParams(collective_id=0, has_side_effects=True),
        name="section",
    )(box_shift, fields_now, parent, advect, diffuse)


def out_kernel(slope, value, slope_hbm, value_hbm, sem):
    copies = [pltpu.make_async_copy(slope, slope_hbm, sem.at[0]), pltpu.make_async_copy(value, value_hbm, sem.at[1])]
    for copy in copies:
        copy.start()
    for copy in copies:
        copy.wait()


def hand_out(slope, value):
    shape = jax.ShapeDtypeStruct(slope.shape, F32)
    hbm = pl.BlockSpec(memory_space=pl.ANY)
    slope, value = [pltpu.with_memory_space_constraint(a, pltpu.VMEM) for a in (slope, value)]
    return pl.pallas_call(
        out_kernel, out_shape=(shape, shape), in_specs=[hbm] * 2, out_specs=(hbm, hbm),
        scratch_shapes=[pltpu.SemaphoreType.DMA((2,))], name="out")(slope, value)


def local(fields_now, parent, advect, diffuse, box_shift):
    return hand_out(*section(fields_now, parent, advect, diffuse, box_shift))


def solution(mesh):
    return jax.shard_map(
        local,
        mesh=mesh,
        in_specs=(P(None, "gx", "gy", "gz"), P(None, "gx", "gy", "gz"), P(), P(), P()),
        out_specs=(P(None, "gx", "gy", "gz"), P(None, "gx", "gy", "gz")),
        check_vma=False,
    )
```
